256 devices in a mesh: exp: 8 (over y, x_hi), dp: 32 (over x_lo, z, core).
Axes of the slice: x: 4 (x_hi: 2, x_lo: 2; x = x_hi * 2 + x_lo), y: 4, z: 8, core: 2. Of those that a mesh axis runs over, the one named last changes fastest.
Arguments:
- expert_inputs: bfloat16 [8, 8192, 2048], P('exp', 'dp'), may hold values from -6 to 6
- hidden_grads: bfloat16 [8, 8192, 7168], P('exp', 'dp'), may hold values from -0.0625 to 0.0625
- expert_weight: float32 [8, 2048, 7168], P('exp', 'dp'), may hold values from -0.125 to 0.125
- expert_moment: bfloat16 [8, 2048, 7168], P('exp', 'dp'), may hold values from -4 to 4
- expert_second: bfloat16 [8, 2048, 7168], P('exp', 'dp'), may hold values from 0.0009994507 to 1
- key_partial: float32 [8, 2048, 512], P('exp', 'dp'), may hold values from -5 to 5
- key_weight: float32 [2048, 512], P('dp'), may hold values from -0.125 to 0.125
- key_moment: float32 [8, 256, 512], P('exp', 'dp'), may hold values from -4 to 4
- key_second: float32 [8, 256, 512], P('exp', 'dp'), may hold values from 0.001 to 1
- slice_owner: int32 [8], replicated, may hold values from 0 to 7, each once
Outputs:
- expert_weight_next: float32 [8, 2048, 7168], P('exp', 'dp')
- expert_moment_next: bfloat16 [8, 2048, 7168], P('exp', 'dp')
- expert_second_next: bfloat16 [8, 2048, 7168], P('exp', 'dp')
- key_weight_next: float32 [2048, 512], P('dp')
- key_moment_next: float32 [8, 256, 512], P('exp', 'dp')
- key_second_next: float32 [8, 256, 512], P('exp', 'dp')
The draws below stay inside these ranges and needn't reach their ends.
Inputs may be any that keep to these rules, and one draw needn't show every extreme that they name: `slice_owner`: each exp group holds exactly one slice.
All inputs are finite; a program needn't handle non-finite values.
Results may differ from the reference program's by a relative error of at most 0.012.
Values may be sent and summed in bfloat16 or wider, within the bound.
No kernel may reach another device: no remote copies, remote signals or barrier semaphores. Data moves between devices by JAX's collectives and lax.ppermute only.
A program may use at most 192 MiB of HBM per device.

```python
import math
import jax
import jax.numpy as jnp
from jax import lax

DW = 2048
FE = 7168
KA = 512
TOK_DEV = 256
STEP = 10
TOKENS = 8192
N_EXP = 8
N_DP = 32


def strengthened(values, key, source, target, blocks, factor):
    def block_of(position):
        return (jnp.arange(values.shape[position]) // (values.shape[position] // blocks)).reshape((-1,) + (1,) * (values.ndim - 1 - position))

    one_side = jax.random.permutation(key, blocks)[block_of(target)]
    far = (block_of(target) + blocks // 2) % blocks
    return jnp.where((block_of(source) == one_side) | (block_of(source) == far), factor * values, values)


def block_scale(rng, shape, shards, low, high):
    factor_of = 1.0
    for axis_at, parts in shards:
        heights = jax.random.uniform(jax.random.fold_in(jax.random.fold_in(rng, 6), axis_at), (parts,), jnp.float32, low / len(shards), high / len(shards))
        factor_of = factor_of * jnp.repeat(jnp.exp(heights), shape[axis_at] // parts).reshape((-1,) + (1,) * (len(shape) - 1 - axis_at))
    return factor_of


def bell_draw(key, dims, deviation, reach, shards=(), kind=jnp.bfloat16):
    factor_of = block_scale(key, dims, shards, -0.22, 0.18) if shards else 1.0
    array = jax.random.normal(key, dims, jnp.float32) * deviation * factor_of
    return jnp.minimum(jnp.maximum(array, -reach), reach).astype(kind)


def gaussian_with(own_key, extent, width, reach, cuts, heavy, kind=jnp.bfloat16):
    entries = width * jax.random.normal(own_key, extent, jnp.float32)
    if cuts:
        entries = entries * block_scale(own_key, extent, cuts, -0.22, 0.18)
    return jnp.clip(strengthened(entries, jax.random.fold_in(own_key, 3), *heavy), -reach, reach).astype(kind)


def setup_inputs(seed: int = 0) -> dict:
    key_of = jax.random.split(jax.random.key(seed), 11)
    return {
        "expert_inputs": gaussian_with(key_of[0], (N_EXP, TOKENS, DW), 1.0, 6.0, ((0, 8), (1, 32)), (1, 2, 32, 2.75)),
        "hidden_grads": bell_draw(key_of[1], (N_EXP, TOKENS, FE), TOKENS ** -0.5, 0.0625, ((0, 8), (1, 32))),
        "expert_weight": bell_draw(key_of[2], (N_EXP, DW, FE), DW ** -0.5, 0.125, ((0, 8), (1, 32)), jnp.float32),
        "expert_moment": bell_draw(key_of[3], (N_EXP, DW, FE), 0.3, 4.0, ((0, 8), (1, 32))),
        "expert_second": jnp.clip(jnp.exp(math.log(1.0) - 6.9083047 * jax.random.uniform(key_of[4], (N_EXP, DW, FE), jnp.float32) ** block_scale(key_of[4], (N_EXP, DW, FE), ((0, 8), (1, 32)), -0.2, 0.2)), 0.0009994507, 1.0).astype(jnp.bfloat16),
        "key_partial": bell_draw(key_of[5], (N_EXP, DW, KA), 0.35, 5.0, ((0, 8), (1, 32)), jnp.float32),
        "key_weight": bell_draw(key_of[6], (DW, KA), DW ** -0.5, 0.125, ((0, 32),), jnp.float32),
        "key_moment": bell_draw(key_of[7], (N_EXP, DW // N_EXP, KA), 0.3, 4.0, ((0, 8), (1, 32)), jnp.float32),
        "key_second": jnp.clip(jnp.exp(math.log(1.0) - 6.9077552 * jax.random.uniform(key_of[8], (N_EXP, DW // N_EXP, KA), jnp.float32) ** block_scale(key_of[8], (N_EXP, DW // N_EXP, KA), ((0, 8), (1, 32)), -0.2, 0.2)), 0.001, 1.0),
        "slice_owner": jax.random.permutation(key_of[9], N_EXP).astype(jnp.int32),
    }


first_decay = 0.9
second_decay = 0.999
learn_rate = 0.01
weight_decay = 0.1
epsilon = 1e-08

def adam_update(param, moment, second, gradient):
    moment_new = first_decay * moment.astype(jnp.float32) + (1.0 - first_decay) * gradient
    second_new = second_decay * second.astype(jnp.float32) + (1.0 - second_decay) * gradient * gradient
    moment_hat = moment_new / (1.0 - first_decay ** STEP)
    second_hat = second_new / (1.0 - second_decay ** STEP)
    param_new = param - learn_rate * (moment_hat / (jnp.sqrt(second_hat) + epsilon) + weight_decay * param)
    return (param_new, moment_new, second_new)

def one_expert(packed):
    inputs, upstream, param, moment, second = packed

    def accumulate(running, block):
        offset = (block * TOK_DEV).astype(jnp.int32)
        rows_in = lax.dynamic_slice_in_dim(inputs, offset, TOK_DEV, 0)
        rows_up = lax.dynamic_slice_in_dim(upstream, offset, TOK_DEV, 0)
        partial_value = lax.dot_general(rows_in, rows_up, (((0,), (0,)), ((), ())), preferred_element_type=jnp.float32)
        partial_value = lax.optimization_barrier(partial_value.astype(jnp.bfloat16)).astype(jnp.float32)
        return (running + partial_value, None)
    gradient, _ = lax.scan(accumulate, jnp.zeros((DW, FE), jnp.float32), jnp.arange(N_DP, dtype=jnp.int32))
    param_new, moment_new, second_new = adam_update(param, moment, second, gradient)
    return (param_new, moment_new.astype(jnp.bfloat16), second_new.astype(jnp.bfloat16))

def reference(expert_inputs, hidden_grads, expert_weight, expert_moment, expert_second, key_partial, key_weight, key_moment, key_second, slice_owner):
    expert_weight_next, expert_moment_next, expert_second_next = lax.map(one_expert, (expert_inputs, hidden_grads, expert_weight, expert_moment, expert_second))
    slice_rows = DW // (N_DP * N_EXP)
    key_gradient = lax.optimization_barrier(jnp.sum(key_partial, axis=0))
    owner = slice_owner.astype(jnp.int32)

    def to_rows(held):
        ordered = held.reshape(N_EXP, N_DP, slice_rows, KA)[owner]
        return jnp.transpose(ordered, (1, 0, 2, 3)).reshape(DW, KA)
    inverse = jnp.zeros((N_EXP,), jnp.int32).at[owner].set(jnp.arange(N_EXP, dtype=jnp.int32))

    def to_held(rows):
        ordered = jnp.transpose(rows.reshape(N_DP, N_EXP, slice_rows, KA), (1, 0, 2, 3))
        return ordered[inverse].reshape(N_EXP, DW // N_EXP, KA)
    key_weight_next, moment_rows, second_rows = adam_update(key_weight, to_rows(key_moment), to_rows(key_second), key_gradient)
    return (expert_weight_next, expert_moment_next, expert_second_next, key_weight_next, to_held(moment_rows), to_held(second_rows))
```

```python
import jax
import jax.numpy as jnp
from jax import lax
from jax.sharding import Mesh, PartitionSpec as P

STEP = 10

first_decay = 0.9
second_decay = 0.999
learn_rate = 0.01
weight_decay = 0.1
epsilon = 1e-08

NEAR = (512, 512)
FAR = (640, 640)


def adam_update(param, moment, second, gradient):
    moment_new = first_decay * moment.astype(jnp.float32) + (1.0 - first_decay) * gradient
    second_new = (
        second_decay * second.astype(jnp.float32) + (1.0 - second_decay) * gradient * gradient
    )
    moment_hat = moment_new / (1.0 - first_decay**STEP)
    second_hat = second_new / (1.0 - second_decay**STEP)
    param_new = param - learn_rate * (
        moment_hat / (jnp.sqrt(second_hat) + epsilon) + weight_decay * param
    )
    return (param_new, moment_new, second_new)


def dot_tokens(inputs, upstream):
    return lax.dot_general(
        inputs, upstream, (((0,), (0,)), ((), ())), preferred_element_type=jnp.float32
    ).astype(jnp.bfloat16)


def key_steps(
    key_partial, key_weight, key_moment, key_second, slice_owner, seq, mark, ordered, result
):
    n_exp = slice_owner.shape[0]
    holder = lax.axis_index("exp")
    shard_rows, columns_key = key_weight.shape
    slice_rows = shard_rows // n_exp
    ids = jnp.arange(n_exp, dtype=jnp.int32)
    bits = [n_exp >> (i + 1) for i in range(n_exp.bit_length() - 1)]
    flags = [(holder // bit) % 2 for bit in bits]
    swaps = [[(e, e ^ bit) for e in range(n_exp)] for bit in bits]
    picker = (slice_owner[None, :] == ids[:, None]).astype(jnp.float32)
    value = jnp.dot(
        picker, seq(key_partial)[0].reshape(n_exp, slice_rows * columns_key),
        precision=lax.Precision.HIGHEST, preferred_element_type=jnp.float32,
    ).reshape((2,) * len(bits) + (slice_rows, columns_key))
    for flag, perm in zip(flags, swaps):
        send = lax.dynamic_index_in_dim(value, 1 - flag, 0, keepdims=False).astype(jnp.bfloat16)
        keep = lax.dynamic_index_in_dim(value, flag, 0, keepdims=False)
        mark(send)
        got = lax.ppermute(send, "exp", perm)
        yield
        value = keep + seq(got).astype(jnp.float32)
    held_slice = jnp.sum(jnp.where(slice_owner == holder, ids, 0))
    old_slice = lax.dynamic_slice_in_dim(key_weight, held_slice * slice_rows, slice_rows, 0)
    value, result["moment"], result["second"] = adam_update(
        old_slice, key_moment[0], key_second[0], value
    )
    for flag, perm in zip(flags[::-1], swaps[::-1]):
        mark(value)
        got = lax.ppermute(value, "exp", perm)
        yield
        value = jnp.stack(ordered(flag, value, seq(got)), 0)
    result["weight"] = jnp.dot(
        picker.T, value.reshape(n_exp, slice_rows * columns_key),
        precision=lax.Precision.HIGHEST, preferred_element_type=jnp.float32,
    ).reshape(shard_rows, columns_key)


def make_shards(n_exp, n_z, n_y):
    swap = [(0, 1), (1, 0)]

    def over_x(value):
        return lax.ppermute(value, "x_lo", swap)

    def over_core(value):
        return lax.ppermute(value, "core", swap)

    up_ring = [(z, (z + 1) % n_z) for z in range(n_z)]
    down_ring = [(z, (z - 1) % n_z) for z in range(n_z)]

    def columns(value, start, size):
        return lax.dynamic_slice_in_dim(value, start, size, 1)

    def shards(
        expert_inputs,
        hidden_grads,
        expert_weight,
        expert_moment,
        expert_second,
        key_partial,
        key_weight,
        key_moment,
        key_second,
        slice_owner,
    ):
        x = lax.axis_index("x_lo")
        z = lax.axis_index("z")
        core = lax.axis_index("core")
        inputs = expert_inputs[0]
        upstream = hidden_grads[0]
        tokens, rows = inputs.shape
        part = rows // (2 * n_z)

        def piece(partial, k):
            blocks = partial.reshape(2, n_z, part, partial.shape[1])
            return lax.dynamic_index_in_dim(blocks, (z + k) % n_z, 1, keepdims=False)

        token = []

        def seq(value):
            return lax.optimization_barrier((value, tuple(token)))[0] if token else value

        def mark(*values):
            token[:] = values

        def ring(partial, lead_up):
            half = n_z // 2
            return {
                "partial": partial,
                "up": list(range(half if lead_up else half - 1, 0, -1)),
                "down": list(range(half - 1 if lead_up else half, 0, -1)),
                "got_up": None,
                "got_down": None,
            }

        def advance(state):
            sent = []
            got = seq((state["got_up"], state["got_down"], state["partial"]))
            for name, value, sign, perm in (
                ("up", got[0], 1, up_ring),
                ("down", got[1], -1, down_ring),
            ):
                if not state[name]:
                    continue
                total = piece(got[2], sign * state[name].pop(0))
                if value is not None:
                    total = total.astype(jnp.float32) + value.astype(jnp.float32)
                    total = total.astype(jnp.bfloat16)
                sent.append(total)
                state["got_" + name] = lax.ppermute(total, "z", perm)
            mark(*sent)

        def finish(state):
            up, down, partial = seq((state["got_up"], state["got_down"], state["partial"]))
            total = piece(partial, 0).astype(jnp.float32)
            return total + up.astype(jnp.float32) + down.astype(jnp.float32)

        def ordered(flag, mine, other):
            return [jnp.where(flag == 0, mine, other), jnp.where(flag == 0, other, mine)]

        half = part // 2

        def rows_for(value, where, dim):
            return lax.dynamic_slice_in_dim(value, where * half, half, dim)

        def near_rows(total):
            total = total.astype(jnp.bfloat16)
            give = lax.dynamic_index_in_dim(total, 1 - x, 0, keepdims=False)
            keep = lax.dynamic_index_in_dim(total, x, 0, keepdims=False)
            mark(give)
            return keep, over_x(give)

        def near_slab(keep, got):
            mine = (keep.astype(jnp.float32) + seq(got).astype(jnp.float32)).astype(jnp.bfloat16)
            give = rows_for(mine, 1 - core, 0)
            mark(give)
            return ordered(core, rows_for(mine, core, 0), over_core(give))

        def far_slab(keep, got):
            pair = jnp.stack([keep, seq(got)], 0)
            give = rows_for(pair, 1 - core, 1)
            mark(give)
            by_core = ordered(core, rows_for(pair, core, 1), over_core(give))
            order = [ordered(x, value[0], value[1]) for value in by_core]
            return [order[0][0], order[1][0], order[0][1], order[1][1]]

        def far_upstream(width, own, sent):
            pair = jnp.stack([own, seq(sent)], 0)
            keep = lax.dynamic_slice_in_dim(pair, core * width, width, 2)
            give = lax.dynamic_slice_in_dim(pair, (1 - core) * width, width, 2)
            mark(give)
            return keep, over_core(give)

        def far_ring(halves, lead_up):
            keep, got = halves
            up = jnp.concatenate([keep[0], got[0], keep[1], got[1]], 0)
            state = ring(dot_tokens(seq(inputs_all), up), lead_up)
            advance(state)
            return state

        key_state = {}
        key = key_steps(
            key_partial, key_weight, key_moment, key_second, slice_owner, seq, mark, ordered,
            key_state,
        )

        near = sum(NEAR)
        inputs_x = over_x(inputs)
        inputs_core = over_core(inputs)
        up_near = columns(upstream, core * near, near)
        up_near_core = over_core(columns(upstream, (1 - core) * near, near))
        inputs_chip = jnp.concatenate([inputs, inputs_core], 0)
        up_chip = jnp.concatenate([up_near, up_near_core], 0)
        near0 = ring(dot_tokens(inputs_chip, up_chip[:, : NEAR[0]]), True)
        advance(near0)
        near1 = ring(dot_tokens(inputs_chip, seq(up_chip)[:, NEAR[0] :]), False)
        advance(near1)

        far_sent = []
        far_own = []
        start = 2 * near
        for width in FAR:
            later = seq(upstream)
            give = columns(later, start + (1 - x) * 2 * width, 2 * width)
            mark(give)
            far_sent.append(over_x(give))
            far_own.append(columns(later, start + x * 2 * width, 2 * width))
            start += 4 * width

        next(key)
        advance(near0)
        advance(near1)
        give = seq(inputs_x)
        inputs_all = jnp.concatenate([inputs_chip, give, over_core(give)], 0)
        next(key)
        advance(near0)
        advance(near1)
        halves = far_upstream(FAR[0], far_own[0], far_sent[0])
        advance(near0)
        advance(near1)
        far0 = far_ring(halves, True)
        near0 = near_rows(finish(near0))
        near1 = near_rows(finish(near1))
        halves = far_upstream(FAR[1], far_own[1], far_sent[1])
        advance(far0)
        next(key)
        far1 = far_ring(halves, False)
        slab0 = near_slab(*near0)
        slab1 = near_slab(*near1)
        advance(far0)
        next(key)
        advance(far1)
        advance(far0)
        next(key)
        advance(far1)
        far0 = near_rows(finish(far0))
        next(key)
        advance(far1)
        slab2 = far_slab(*far0)
        next(key, None)
        far1 = near_rows(finish(far1))
        slab3 = far_slab(*far1)

        slices = [slab0[0], slab1[0], slab0[1], slab1[1], *slab2, *slab3]
        gradient = jnp.concatenate(slices, 1).astype(jnp.float32)
        weight_next, moment_f, second_f = adam_update(
            expert_weight[0], expert_moment[0], expert_second[0], gradient
        )
        return (
            weight_next[None],
            moment_f.astype(jnp.bfloat16)[None],
            second_f.astype(jnp.bfloat16)[None],
            key_state["weight"],
            key_state["moment"][None],
            key_state["second"][None],
        )

    return shards


def solution(mesh):
    n_exp = mesh.shape["exp"]
    n_z = mesh.shape["dp"] // 4
    inner = Mesh(
        mesh.devices.reshape(n_exp, 2, n_z, 2), ("exp", "x_lo", "z", "core")
    )
    dp = ("x_lo", "z", "core")
    wide = P("exp", dp, None)
    in_specs = (wide,) * 6 + (P(dp, None), wide, wide, P())
    out_specs = (wide, wide, wide, P(dp, None), wide, wide)
    return jax.shard_map(
        make_shards(n_exp, n_z, n_exp // 2), mesh=inner, in_specs=in_specs, out_specs=out_specs,
        check_vma=False,
    )
```

```python
import jax
import jax.numpy as jnp
from jax import lax
from jax.sharding import Mesh, PartitionSpec as P

STEP = 10

first_decay = 0.9
second_decay = 0.999
learn_rate = 0.01
weight_decay = 0.1
epsilon = 1e-08

NEAR = (512, 512)
FAR = (640, 640)


def adam_update(param, moment, second, gradient):
    moment_new = first_decay * moment.astype(jnp.float32) + (1.0 - first_decay) * gradient
    second_new = (
        second_decay * second.astype(jnp.float32) + (1.0 - second_decay) * gradient * gradient
    )
    moment_hat = moment_new / (1.0 - first_decay**STEP)
    second_hat = second_new / (1.0 - second_decay**STEP)
    param_new = param - learn_rate * (
        moment_hat / (jnp.sqrt(second_hat) + epsilon) + weight_decay * param
    )
    return (param_new, moment_new, second_new)


def dot_tokens(inputs, upstream):
    return lax.dot_general(
        inputs, upstream, (((0,), (0,)), ((), ())), preferred_element_type=jnp.float32
    ).astype(jnp.bfloat16)


def key_steps(
    key_partial, key_weight, key_moment, key_second, slice_owner, seq, mark, ordered, result
):
    n_exp = slice_owner.shape[0]
    holder = lax.axis_index("exp")
    shard_rows, columns_key = key_weight.shape
    slice_rows = shard_rows // n_exp
    ids = jnp.arange(n_exp, dtype=jnp.int32)
    bits = [n_exp >> (i + 1) for i in range(n_exp.bit_length() - 1)]
    flags = [(holder // bit) % 2 for bit in bits]
    swaps = [[(e, e ^ bit) for e in range(n_exp)] for bit in bits]
    picker = (slice_owner[None, :] == ids[:, None]).astype(jnp.float32)
    value = jnp.dot(
        picker, seq(key_partial)[0].reshape(n_exp, slice_rows * columns_key),
        precision=lax.Precision.HIGHEST, preferred_element_type=jnp.float32,
    ).reshape((2,) * len(bits) + (slice_rows, columns_key))
    for flag, perm in zip(flags, swaps):
        send = lax.dynamic_index_in_dim(value, 1 - flag, 0, keepdims=False).astype(jnp.bfloat16)
        keep = lax.dynamic_index_in_dim(value, flag, 0, keepdims=False)
        mark(send)
        got = lax.ppermute(send, "exp", perm)
        yield
        value = keep + seq(got).astype(jnp.float32)
    held_slice = jnp.sum(jnp.where(slice_owner == holder, ids, 0))
    old_slice = lax.dynamic_slice_in_dim(key_weight, held_slice * slice_rows, slice_rows, 0)
    value, result["moment"], result["second"] = adam_update(
        old_slice, key_moment[0], key_second[0], value
    )
    for flag, perm in zip(flags[::-1], swaps[::-1]):
        mark(value)
        got = lax.ppermute(value, "exp", perm)
        yield
        value = jnp.stack(ordered(flag, value, seq(got)), 0)
    result["weight"] = jnp.dot(
        picker.T, value.reshape(n_exp, slice_rows * columns_key),
        precision=lax.Precision.HIGHEST, preferred_element_type=jnp.float32,
    ).reshape(shard_rows, columns_key)


def make_shards(n_exp, n_z, n_y):
    swap = [(0, 1), (1, 0)]

    def over_x(value):
        return lax.ppermute(value, "x_lo", swap)

    def over_core(value):
        return lax.ppermute(value, "core", swap)

    up_ring = [(z, (z + 1) % n_z) for z in range(n_z)]
    down_ring = [(z, (z - 1) % n_z) for z in range(n_z)]

    def columns(value, start, size):
        return lax.dynamic_slice_in_dim(value, start, size, 1)

    def shards(
        expert_inputs,
        hidden_grads,
        expert_weight,
        expert_moment,
        expert_second,
        key_partial,
        key_weight,
        key_moment,
        key_second,
        slice_owner,
    ):
        x = lax.axis_index("x_lo")
        z = lax.axis_index("z")
        core = lax.axis_index("core")
        inputs = expert_inputs[0]
        upstream = hidden_grads[0]
        tokens, rows = inputs.shape
        part = rows // (2 * n_z)

        def piece(partial, k):
            blocks = partial.reshape(2, n_z, part, partial.shape[1])
            return lax.dynamic_index_in_dim(blocks, (z + k) % n_z, 1, keepdims=False)

        token = []

        def seq(value):
            return lax.optimization_barrier((value, tuple(token)))[0] if token else value

        def mark(*values):
            token[:] = values

        def ring(partial, lead_up):
            half = n_z // 2
            return {
                "partial": partial,
                "up": list(range(half if lead_up else half - 1, 0, -1)),
                "down": list(range(half - 1 if lead_up else half, 0, -1)),
                "got_up": None,
                "got_down": None,
            }

        def advance(state):
            sent = []
            got = seq((state["got_up"], state["got_down"], state["partial"]))
            for name, value, sign, perm in (
                ("up", got[0], 1, up_ring),
                ("down", got[1], -1, down_ring),
            ):
                if not state[name]:
                    continue
                total = piece(got[2], sign * state[name].pop(0))
                if value is not None:
                    total = total.astype(jnp.float32) + value.astype(jnp.float32)
                    total = total.astype(jnp.bfloat16)
                sent.append(total)
                state["got_" + name] = lax.ppermute(total, "z", perm)
            mark(*sent)

        def finish(state):
            up, down, partial = seq((state["got_up"], state["got_down"], state["partial"]))
            total = piece(partial, 0).astype(jnp.float32)
            return total + up.astype(jnp.float32) + down.astype(jnp.float32)

        def ordered(flag, mine, other):
            return [jnp.where(flag == 0, mine, other), jnp.where(flag == 0, other, mine)]

        half = part // 2

        def rows_for(value, where, dim):
            return lax.dynamic_slice_in_dim(value, where * half, half, dim)

        def near_rows(total):
            total = total.astype(jnp.bfloat16)
            give = lax.dynamic_index_in_dim(total, 1 - x, 0, keepdims=False)
            keep = lax.dynamic_index_in_dim(total, x, 0, keepdims=False)
            mark(give)
            return keep, over_x(give)

        def near_slab(keep, got):
            mine = (keep.astype(jnp.float32) + seq(got).astype(jnp.float32)).astype(jnp.bfloat16)
            give = rows_for(mine, 1 - core, 0)
            mark(give)
            return ordered(core, rows_for(mine, core, 0), over_core(give))

        def far_slab(keep, got):
            pair = jnp.stack([keep, seq(got)], 0)
            give = rows_for(pair, 1 - core, 1)
            mark(give)
            by_core = ordered(core, rows_for(pair, core, 1), over_core(give))
            order = [ordered(x, value[0], value[1]) for value in by_core]
            return [order[0][0], order[1][0], order[0][1], order[1][1]]

        def far_upstream(width, own, sent):
            pair = jnp.stack([own, seq(sent)], 0)
            keep = lax.dynamic_slice_in_dim(pair, core * width, width, 2)
            give = lax.dynamic_slice_in_dim(pair, (1 - core) * width, width, 2)
            mark(give)
            return keep, over_core(give)

        def far_ring(halves, lead_up):
            keep, got = halves
            up = jnp.concatenate([keep[0], got[0], keep[1], got[1]], 0)
            state = ring(dot_tokens(seq(inputs_all), up), lead_up)
            advance(state)
            return state

        key_state = {}
        key = key_steps(
            key_partial, key_weight, key_moment, key_second, slice_owner, seq, mark, ordered,
            key_state,
        )

        near = sum(NEAR)
        inputs_x = over_x(inputs)
        inputs_core = over_core(inputs)
        up_near = columns(upstream, core * near, near)
        up_near_core = over_core(columns(upstream, (1 - core) * near, near))
        inputs_chip = jnp.concatenate([inputs, inputs_core], 0)
        up_chip = jnp.concatenate([up_near, up_near_core], 0)
        near0 = ring(dot_tokens(inputs_chip, up_chip[:, : NEAR[0]]), True)
        advance(near0)
        near1 = ring(dot_tokens(inputs_chip, seq(up_chip)[:, NEAR[0] :]), False)
        advance(near1)

        far_sent = []
        far_own = []
        start = 2 * near
        for width in FAR:
            later = seq(upstream)
            give = columns(later, start + (1 - x) * 2 * width, 2 * width)
            mark(give)
            far_sent.append(over_x(give))
            far_own.append(columns(later, start + x * 2 * width, 2 * width))
            start += 4 * width

        next(key)
        advance(near0)
        advance(near1)
        give = seq(inputs_x)
        inputs_all = jnp.concatenate([inputs_chip, give, over_core(give)], 0)
        next(key)
        advance(near0)
        advance(near1)
        halves = far_upstream(FAR[0], far_own[0], far_sent[0])
        advance(near0)
        advance(near1)
        far0 = far_ring(halves, True)
        near0 = near_rows(jnp.concatenate([finish(near0), finish(near1)], 2))
        halves = far_upstream(FAR[1], far_own[1], far_sent[1])
        advance(far0)
        next(key)
        far1 = far_ring(halves, False)
        slab0 = near_slab(*near0)
        advance(far0)
        next(key)
        advance(far1)
        advance(far0)
        next(key)
        advance(far1)
        far0 = near_rows(finish(far0))
        next(key)
        advance(far1)
        slab2 = far_slab(*far0)
        next(key, None)
        far1 = near_rows(finish(far1))
        slab3 = far_slab(*far1)

        slices = [*slab0, *slab2, *slab3]
        gradient = jnp.concatenate(slices, 1).astype(jnp.float32)
        weight_next, moment_f, second_f = adam_update(
            expert_weight[0], expert_moment[0], expert_second[0], gradient
        )
        return (
            weight_next[None],
            moment_f.astype(jnp.bfloat16)[None],
            second_f.astype(jnp.bfloat16)[None],
            key_state["weight"],
            key_state["moment"][None],
            key_state["second"][None],
        )

    return shards


def solution(mesh):
    n_exp = mesh.shape["exp"]
    n_z = mesh.shape["dp"] // 4
    inner = Mesh(
        mesh.devices.reshape(n_exp, 2, n_z, 2), ("exp", "x_lo", "z", "core")
    )
    dp = ("x_lo", "z", "core")
    wide = P("exp", dp, None)
    in_specs = (wide,) * 6 + (P(dp, None), wide, wide, P())
    out_specs = (wide, wide, wide, P(dp, None), wide, wide)
    return jax.shard_map(
        make_shards(n_exp, n_z, n_exp // 2), mesh=inner, in_specs=in_specs, out_specs=out_specs,
        check_vma=False,
    )
```
